32 devices in a mesh: data: 2 (over x), cp: 4 (over z), tp: 4 (over y, core).
Axes of the slice: x: 2, y: 2, z: 4, core: 2. Of those that a mesh axis runs over, the one named last changes fastest.
Arguments:
- act_in: bfloat16 [2, 6144, 3584], P(None, ('data', 'cp', 'tp')), parts along dimension 1
- route_ids: int32 [2, 6144, 2], P(None, ('data', 'cp', 'tp')), parts along dimension 1
- route_gates: float32 [2, 6144, 2], P(None, ('data', 'cp', 'tp')), parts along dimension 1
- w_query: bfloat16 [3584, 28, 128], P(None, 'tp')
- w_key: bfloat16 [3584, 4, 128], P(None, 'tp')
- w_value: bfloat16 [3584, 4, 128], P(None, 'tp')
- w_out: bfloat16 [28, 128, 3584], P('tp')
- w_gate: bfloat16 [16, 3584, 2560], P(('cp', 'tp'))
- w_up: bfloat16 [16, 3584, 2560], P(('cp', 'tp'))
- w_down: bfloat16 [16, 2560, 3584], P(('cp', 'tp'))
Outputs:
- output: bfloat16 [2, 6144, 3584], P(None, ('data', 'cp', 'tp')), parts along dimension 1
There are 2 independent parts. The reference program is written for one: setup_inputs(seed, part) draws one part's arguments, and reference() takes and returns one part's arrays. A program takes and returns all parts, laid end to end along the dimension named above; an argument that names none is the same for every part.
All inputs are finite; a program needn't handle non-finite values.
Results may differ from the reference program's by a relative error of at most 0.00542754.
Values are sent between devices in bfloat16 or wider.
A program may use at most 1 GiB of HBM per device.

```python
import math
import jax
import jax.numpy as jnp
from jax import lax

HIDDEN = 3584
EXPERT_FF = 2560
Q_HEADS = 28
KV_HEADS = 4
HEAD_DIM = 128
CP_SIZE = 4
TP_SIZE = 4
TOKENS_DEV = 192
MICRO_BATCHES = 2

EXPERTS = CP_SIZE * TP_SIZE
SEQ_LEN = TOKENS_DEV * EXPERTS
PIECE_LEN = SEQ_LEN // (2 * CP_SIZE)
CAPACITY = (4 * TOKENS_DEV) // EXPERTS
EXPERT_ROWS = CAPACITY * EXPERTS
GROUP_SIZE = Q_HEADS // KV_HEADS
SCORE_SHARP = math.sqrt(0.75 * math.log(SEQ_LEN))


def draw_routing(base_key):
    half_cap = CAPACITY // 2

    def one_source(src_key):
        k_perm, k_delta, k_tok, k_swap = jax.random.split(src_key, 4)
        expert_perm = jax.random.permutation(k_perm, EXPERTS)
        deltas = jax.random.randint(k_delta, (EXPERTS // 2,), 0, half_cap + 1).at[0].set(half_cap)
        pair_counts = jnp.stack([half_cap + deltas, half_cap - deltas], axis=1).reshape(EXPERTS)
        counts = jnp.zeros((EXPERTS,), jnp.int32).at[expert_perm].set(pair_counts)
        count_ends = jnp.cumsum(counts)
        labels = jnp.sum((jnp.arange(2 * TOKENS_DEV)[:, None] >= count_ends[None, :]).astype(jnp.int32), axis=1)
        id_pairs = jnp.stack([labels[:TOKENS_DEV], labels[TOKENS_DEV:]], axis=1)
        id_pairs = id_pairs[jax.random.permutation(k_tok, TOKENS_DEV)]
        swap_flag = jax.random.randint(k_swap, (TOKENS_DEV, 1), 0, 2)
        return jnp.where(swap_flag == 1, id_pairs[:, ::-1], id_pairs).astype(jnp.int32)

    return jax.vmap(one_source)(jax.random.split(base_key, EXPERTS)).reshape(SEQ_LEN, 2)


def normal_weight(weight_key, arr_shape, w_scale):
    return (jax.random.normal(weight_key, arr_shape, jnp.float32) * w_scale).astype(jnp.bfloat16)


def expert_stack(weight_key, arr_shape, w_scale):
    return lax.map(lambda one_key: normal_weight(one_key, arr_shape, w_scale), jax.random.split(weight_key, EXPERTS))


def setup_inputs(seed: int = 0, part: int = 0) -> dict:
    part_key = jax.random.fold_in(jax.random.key(seed), part)
    k_act, k_route, k_gate = jax.random.split(part_key, 3)
    shared = jax.random.split(jax.random.key(seed + 1), 7)
    act_in = jax.random.normal(k_act, (MICRO_BATCHES, SEQ_LEN, HIDDEN), jnp.float32).astype(jnp.bfloat16)
    route_ids = jax.vmap(draw_routing)(jax.random.split(k_route, MICRO_BATCHES))
    route_gates = jax.random.uniform(k_gate, (MICRO_BATCHES, SEQ_LEN, 2), jnp.float32, 0.3, 0.7)
    return {
        'act_in': act_in,
        'route_ids': route_ids,
        'route_gates': route_gates,
        'w_query': normal_weight(shared[0], (HIDDEN, Q_HEADS, HEAD_DIM), SCORE_SHARP / math.sqrt(HIDDEN)),
        'w_key': normal_weight(shared[1], (HIDDEN, KV_HEADS, HEAD_DIM), 1.0 / math.sqrt(HIDDEN)),
        'w_value': normal_weight(shared[2], (HIDDEN, KV_HEADS, HEAD_DIM), 1.0 / math.sqrt(HIDDEN)),
        'w_out': normal_weight(shared[3], (Q_HEADS, HEAD_DIM, HIDDEN), 1.0 / math.sqrt(Q_HEADS * HEAD_DIM)),
        'w_gate': expert_stack(shared[4], (HIDDEN, EXPERT_FF), 1.0 / math.sqrt(HIDDEN)),
        'w_up': expert_stack(shared[5], (HIDDEN, EXPERT_FF), 1.0 / math.sqrt(HIDDEN)),
        'w_down': expert_stack(shared[6], (EXPERT_FF, HIDDEN), 1.0 / math.sqrt(EXPERT_FF)),
    }


def token_positions():
    row_ix = jnp.arange(SEQ_LEN)
    owner_ix = row_ix // (2 * PIECE_LEN)
    inner_ix = row_ix % (2 * PIECE_LEN)
    return jnp.where(inner_ix < PIECE_LEN, owner_ix * PIECE_LEN + inner_ix, (2 * CP_SIZE - 1 - owner_ix) * PIECE_LEN + inner_ix - PIECE_LEN)


def attention_block(seq_in, w_query, w_key, w_value, w_out):
    query_rows = jnp.dot(seq_in, w_query.reshape(HIDDEN, Q_HEADS * HEAD_DIM), preferred_element_type=jnp.float32).astype(jnp.bfloat16)
    key_rows = jnp.dot(seq_in, w_key.reshape(HIDDEN, KV_HEADS * HEAD_DIM), preferred_element_type=jnp.float32).astype(jnp.bfloat16)
    value_rows = jnp.dot(seq_in, w_value.reshape(HIDDEN, KV_HEADS * HEAD_DIM), preferred_element_type=jnp.float32).astype(jnp.bfloat16)
    key_rows = key_rows.astype(jnp.float32).reshape(SEQ_LEN, KV_HEADS, HEAD_DIM)
    value_rows = value_rows.astype(jnp.float32).reshape(SEQ_LEN, KV_HEADS, HEAD_DIM)
    positions = token_positions()
    query_blocks = query_rows.reshape(EXPERTS, TOKENS_DEV, KV_HEADS, GROUP_SIZE, HEAD_DIM)
    pos_blocks = positions.reshape(EXPERTS, TOKENS_DEV)

    def one_block(block_args):
        q_block, q_pos = block_args
        scores = jnp.einsum('qhgd,khd->hgqk', q_block.astype(jnp.float32), key_rows) * HEAD_DIM ** -0.5
        scores = jnp.where(positions[None, :] <= q_pos[:, None], scores, -jnp.inf)
        row_peak = jnp.max(scores, axis=-1, keepdims=True)
        exp_scores = jnp.exp(scores - row_peak)
        row_sum = jnp.sum(exp_scores, axis=-1)
        weighted = jnp.einsum('hgqk,khd->qhgd', exp_scores.astype(jnp.bfloat16).astype(jnp.float32), value_rows)
        weighted = weighted / jnp.transpose(row_sum, (2, 0, 1))[..., None]
        return weighted.astype(jnp.bfloat16).reshape(TOKENS_DEV, Q_HEADS * HEAD_DIM)

    attn_rows = lax.map(one_block, (query_blocks, pos_blocks)).reshape(SEQ_LEN, Q_HEADS * HEAD_DIM)
    attn_sum = jnp.dot(attn_rows, w_out.reshape(Q_HEADS * HEAD_DIM, HIDDEN), preferred_element_type=jnp.float32)
    return (seq_in.astype(jnp.float32) + attn_sum).astype(jnp.bfloat16)


def expert_block(mid_rows, seq_ids, seq_gates, w_gate, w_up, w_down):
    choice_expert = seq_ids.reshape(2 * SEQ_LEN)
    choice_token = jnp.arange(2 * SEQ_LEN) // 2
    sort_ix = jnp.argsort(choice_expert, stable=True)
    counts = jnp.sum((choice_expert[None, :] == jnp.arange(EXPERTS)[:, None]).astype(jnp.int32), axis=1)
    starts = jnp.cumsum(counts) - counts
    sorted_token = jnp.concatenate([choice_token[sort_ix], jnp.zeros((EXPERT_ROWS,), choice_token.dtype)])

    def one_expert(expert_id):
        token_ids = lax.dynamic_slice(sorted_token, (starts[expert_id],), (EXPERT_ROWS,))
        expert_in = mid_rows[token_ids]
        gate_act = jnp.dot(expert_in, w_gate[expert_id], preferred_element_type=jnp.float32)
        up_act = jnp.dot(expert_in, w_up[expert_id], preferred_element_type=jnp.float32)
        mixed_act = (jax.nn.silu(gate_act) * up_act).astype(jnp.bfloat16)
        return jnp.dot(mixed_act, w_down[expert_id], preferred_element_type=jnp.float32).astype(jnp.bfloat16)

    expert_out = lax.map(one_expert, jnp.arange(EXPERTS)).reshape(EXPERTS * EXPERT_ROWS, HIDDEN)
    sorted_expert = choice_expert[sort_ix]
    slot_rank = jnp.arange(2 * SEQ_LEN) - starts[sorted_expert]
    z_sorted = expert_out[sorted_expert * EXPERT_ROWS + slot_rank]
    z_choice = z_sorted[jnp.argsort(sort_ix)].reshape(SEQ_LEN, 2, HIDDEN)
    mixed_sum = jnp.sum(seq_gates[:, :, None] * z_choice.astype(jnp.float32), axis=1)
    return (mid_rows.astype(jnp.float32) + mixed_sum).astype(jnp.bfloat16)


def reference(act_in, route_ids, route_gates, w_query, w_key, w_value, w_out, w_gate, w_up, w_down):
    def one_sequence(seq_args):
        seq_in, seq_ids, seq_gates = seq_args
        mid_rows = attention_block(seq_in, w_query, w_key, w_value, w_out)
        return expert_block(mid_rows, seq_ids, seq_gates, w_gate, w_up, w_down)

    return lax.map(one_sequence, (act_in, route_ids, route_gates))
```

```python
import jax
import jax.numpy as jnp
from jax import lax
from jax.experimental import pallas as pl
from jax.experimental.pallas import tpu as pltpu
from jax.sharding import PartitionSpec as P

F32, BF16 = jnp.float32, jnp.bfloat16


def attend_kernel(cp_size, heads, rank_ref, q_ref, kv_ref, o_ref, vt_ref, acc_ref):
    piece, dim = q_ref.shape[0] // 2, q_ref.shape[1] // heads
    pieces = 2 * cp_size
    scale = dim ** -0.5
    for j in range(pieces):
        owner, half = (j, 0) if j < cp_size else (pieces - 1 - j, 1)
        vt_ref[j] = kv_ref[owner, half * piece:(half + 1) * piece, dim:].T
    rank = rank_ref[0]

    def keys_of(j):
        owner = jnp.where(j < cp_size, j, pieces - 1 - j)
        start = jnp.where(j < cp_size, 0, piece)
        return kv_ref[owner, pl.ds(pl.multiple_of(start, piece), piece), 0:dim]

    for half in range(2):
        last = rank if half == 0 else pieces - 1 - rank
        rows = slice(half * piece, (half + 1) * piece)
        for first in range(0, heads, 2):
            group = range(first, min(first + 2, heads))
            cols = len(group) * piece
            qt = jnp.concatenate([q_ref[rows, n * dim:(n + 1) * dim].T for n in group], axis=1)
            key_ix = lax.broadcasted_iota(jnp.int32, (piece, piece), 0)
            query_ix = lax.broadcasted_iota(jnp.int32, (piece, piece), 1)
            keep = key_ix <= query_ix
            if len(group) == 2:
                keep = jnp.concatenate([keep, keep], axis=1)
            s = jnp.dot(keys_of(last), qt, preferred_element_type=F32) * scale
            s = jnp.where(keep, s, -jnp.inf)
            peak = jnp.max(s, axis=0, keepdims=True)
            e = jnp.exp(s - peak)
            total = jnp.sum(e, axis=0, keepdims=True)
            acc_ref[:, 0:cols] = jnp.dot(vt_ref[last], e.astype(BF16), preferred_element_type=F32)

            def step(j, carry):
                peak, total = carry
                s = jnp.dot(keys_of(j), qt, preferred_element_type=F32) * scale
                new_peak = jnp.maximum(peak, jnp.max(s, axis=0, keepdims=True))
                e = jnp.exp(s - new_peak)
                shrink = jnp.exp(peak - new_peak)
                total = total * shrink + jnp.sum(e, axis=0, keepdims=True)
                acc_ref[:, 0:cols] = acc_ref[:, 0:cols] * shrink + jnp.dot(vt_ref[j], e.astype(BF16), preferred_element_type=F32)
                return new_peak, total

            peak, total = lax.fori_loop(0, last, step, (peak, total))
            out = (acc_ref[:, 0:cols] / total).T.astype(BF16)
            for k, n in enumerate(group):
                o_ref[rows, n * dim:(n + 1) * dim] = out[k * piece:(k + 1) * piece]


def attend(rank, q, kv, cp_size, heads):
    rows, width = q.shape
    dim = width // heads
    vmem = pl.BlockSpec(memory_space=pltpu.VMEM)
    pairs = heads * (rows // 2) ** 2 * (2 * cp_size + 1)
    return pl.pallas_call(
        lambda *refs: attend_kernel(cp_size, heads, *refs),
        out_shape=jax.ShapeDtypeStruct(q.shape, BF16),
        in_specs=[pl.BlockSpec(memory_space=pltpu.SMEM), vmem, vmem],
        out_specs=vmem,
        scratch_shapes=[pltpu.VMEM((2 * cp_size, dim, rows // 2), BF16), pltpu.VMEM((dim, rows), F32)],
        cost_estimate=pl.CostEstimate(flops=6 * dim * pairs, bytes_accessed=4 * q.size + 2 * kv.size, transcendentals=pairs),
        compiler_params=pltpu.CompilerParams(vmem_limit_bytes=24 * 2 ** 20),
    )(rank, q, kv)


def dot(a, b, out=F32):
    return jnp.dot(a, b, preferred_element_type=F32).astype(out)


def solution(mesh):
    cp_size = mesh.shape['cp']
    tp_size = mesh.shape['tp']
    experts = cp_size * tp_size
    row_spec = P(None, ('data', 'cp', 'tp'), None)
    head_spec = P(None, 'tp', None)
    out_spec = P('tp', None, None)
    expert_spec = P(('cp', 'tp'), None, None)
    group = ('cp', 'tp')

    def device_step(act_in, route_ids, route_gates, w_query, w_key, w_value, w_out, w_gate, w_up, w_down):
        n_micro, tokens, hidden = act_in.shape
        heads, dim = w_query.shape[1], w_query.shape[2]
        rank = lax.axis_index('cp')[None].astype(jnp.int32)
        wq = w_query.reshape(hidden, heads * dim)
        wkv = jnp.concatenate([w_key.reshape(hidden, dim), w_value.reshape(hidden, dim)], axis=1)
        wo = w_out.reshape(heads * dim, hidden)

        choices = 2 * tokens
        capacity = 2 * choices // experts
        flat_ids = route_ids.reshape(n_micro, choices)
        hits = (flat_ids[..., None] == jnp.arange(experts)).astype(jnp.int32)
        slot_rank = jnp.cumsum(hits, axis=1) - 1
        slots = (flat_ids * capacity + jnp.sum(slot_rank * hits, axis=-1)).reshape(n_micro, tokens, 2)
        slot_ix = jnp.arange(experts * capacity)

        mids = []
        for b in range(n_micro):
            x_half = lax.all_gather(act_in[b], 'tp', axis=0, tiled=True)
            kv = dot(x_half, wkv, BF16)
            q = dot(x_half, wq, BF16)
            kv_all = lax.all_gather(kv, 'cp', axis=0)
            o = attend(rank, q, kv_all, cp_size, heads)
            attn_sum = lax.psum_scatter(dot(o, wo), 'tp', scatter_dimension=0, tiled=True)
            mids.append((act_in[b].astype(F32) + attn_sum).astype(BF16))

        outs = []
        for b in range(n_micro):
            mid = mids[b]
            pick = ((slots[b, :, 0][None, :] == slot_ix[:, None]) | (slots[b, :, 1][None, :] == slot_ix[:, None])).astype(BF16)
            send = dot(pick, mid, BF16)
            expert_in = lax.all_to_all(send, group, 0, 0, tiled=True)
            gate_act = dot(expert_in, w_gate[0])
            up_act = dot(expert_in, w_up[0])
            mixed = (jax.nn.silu(gate_act) * up_act).astype(BF16)
            expert_out = dot(mixed, w_down[0], BF16)
            back = lax.all_to_all(expert_out, group, 0, 0, tiled=True)
            z0 = dot((slots[b, :, 0][:, None] == slot_ix[None, :]).astype(BF16), back)
            z1 = dot((slots[b, :, 1][:, None] == slot_ix[None, :]).astype(BF16), back)
            gates = route_gates[b]
            outs.append((mid.astype(F32) + gates[:, 0:1] * z0 + gates[:, 1:2] * z1).astype(BF16))
        return jnp.stack(outs)

    return jax.shard_map(device_step, mesh=mesh, in_specs=(row_spec, row_spec, row_spec, head_spec, head_spec, head_spec, out_spec, expert_spec, expert_spec, expert_spec), out_specs=row_spec, check_vma=False)
```

```python
import jax
import jax.numpy as jnp
from jax import lax
from jax.experimental import pallas as pl
from jax.experimental.pallas import tpu as pltpu
from jax.sharding import PartitionSpec as P


F32, BF16 = jnp.float32, jnp.bfloat16


def attend_kernel(cp_size, heads, rank_ref, q_ref, kv_ref, o_ref, vt_ref, acc_ref):
    piece, dim = q_ref.shape[0] // 2, q_ref.shape[1] // heads
    pieces = 2 * cp_size
    scale = dim ** -0.5
    for j in range(pieces):
        owner, half = (j, 0) if j < cp_size else (pieces - 1 - j, 1)
        vt_ref[j] = kv_ref[owner, half * piece:(half + 1) * piece, dim:].T
    rank = rank_ref[0]

    def keys_of(j):
        owner = jnp.where(j < cp_size, j, pieces - 1 - j)
        start = jnp.where(j < cp_size, 0, piece)
        return kv_ref[owner, pl.ds(pl.multiple_of(start, piece), piece), 0:dim]

    for half in range(2):
        last = rank if half == 0 else pieces - 1 - rank
        rows = slice(half * piece, (half + 1) * piece)
        for first in range(0, heads, 2):
            group = range(first, min(first + 2, heads))
            cols = len(group) * piece
            qt = jnp.concatenate([q_ref[rows, n * dim:(n + 1) * dim].T for n in group], axis=1)
            key_ix = lax.broadcasted_iota(jnp.int32, (piece, piece), 0)
            query_ix = lax.broadcasted_iota(jnp.int32, (piece, piece), 1)
            keep = key_ix <= query_ix
            if len(group) == 2:
                keep = jnp.concatenate([keep, keep], axis=1)
            s = jnp.dot(keys_of(last), qt, preferred_element_type=F32) * scale
            s = jnp.where(keep, s, -jnp.inf)
            peak = jnp.max(s, axis=0, keepdims=True)
            e = jnp.exp(s - peak)
            total = jnp.sum(e, axis=0, keepdims=True)
            acc_ref[:, 0:cols] = jnp.dot(vt_ref[last], e.astype(BF16), preferred_element_type=F32)

            def step(j, carry):
                peak, total = carry
                s = jnp.dot(keys_of(j), qt, preferred_element_type=F32) * scale
                new_peak = jnp.maximum(peak, jnp.max(s, axis=0, keepdims=True))
                e = jnp.exp(s - new_peak)
                shrink = jnp.exp(peak - new_peak)
                total = total * shrink + jnp.sum(e, axis=0, keepdims=True)
                acc_ref[:, 0:cols] = acc_ref[:, 0:cols] * shrink + jnp.dot(vt_ref[j], e.astype(BF16), preferred_element_type=F32)
                return new_peak, total

            peak, total = lax.fori_loop(0, last, step, (peak, total))
            out = (acc_ref[:, 0:cols] / total).T.astype(BF16)
            for k, n in enumerate(group):
                o_ref[rows, n * dim:(n + 1) * dim] = out[k * piece:(k + 1) * piece]


def attend(rank, q, kv, cp_size, heads):
    rows, width = q.shape
    dim = width // heads
    vmem = pl.BlockSpec(memory_space=pltpu.VMEM)
    pairs = heads * (rows // 2) ** 2 * (2 * cp_size + 1)
    return pl.pallas_call(
        lambda *refs: attend_kernel(cp_size, heads, *refs),
        out_shape=jax.ShapeDtypeStruct(q.shape, BF16),
        in_specs=[pl.BlockSpec(memory_space=pltpu.SMEM), vmem, vmem],
        out_specs=vmem,
        scratch_shapes=[pltpu.VMEM((2 * cp_size, dim, rows // 2), BF16), pltpu.VMEM((dim, rows), F32)],
        cost_estimate=pl.CostEstimate(flops=6 * dim * pairs, bytes_accessed=4 * q.size + 2 * kv.size, transcendentals=pairs),
        compiler_params=pltpu.CompilerParams(vmem_limit_bytes=24 * 2 ** 20),
    )(rank, q, kv)


def dot(a, b, out=F32):
    return jnp.dot(a, b, preferred_element_type=F32).astype(out)


def after(value, *first):
    return lax.optimization_barrier((value,) + first)[0]


def solution(mesh):
    cp_size = mesh.shape['cp']
    tp_size = mesh.shape['tp']
    experts = cp_size * tp_size
    row_spec = P(None, ('data', 'cp', 'tp'), None)
    head_spec = P(None, 'tp', None)
    out_spec = P('tp', None, None)
    expert_spec = P(('cp', 'tp'), None, None)
    group = ('cp', 'tp')

    def device_step(act_in, route_ids, route_gates, w_query, w_key, w_value, w_out, w_gate, w_up, w_down):
        n_micro, tokens, hidden = act_in.shape
        heads, dim = w_query.shape[1], w_query.shape[2]
        rank = lax.axis_index('cp')[None].astype(jnp.int32)
        wq = w_query.reshape(hidden, heads * dim)
        wkv = jnp.concatenate([w_key.reshape(hidden, dim), w_value.reshape(hidden, dim)], axis=1)
        wo = w_out.reshape(heads * dim, hidden)

        choices = 2 * tokens
        near_n = experts // 2
        capacity = 4 * choices // experts
        half_id = lax.axis_index('cp') // (cp_size // 2)
        swap = [(i, (i + cp_size // 2) % cp_size) for i in range(cp_size)]
        peer_ids = lax.ppermute(route_ids, 'cp', swap)
        pair_ids = jnp.concatenate([route_ids, peer_ids], axis=1)
        peer_gates = lax.ppermute(route_gates, 'cp', swap)
        near_ids = pair_ids.reshape(n_micro, 2 * choices) - half_id * near_n
        hits = (near_ids[..., None] == jnp.arange(near_n)).astype(jnp.int32)
        slot_rank = jnp.cumsum(hits, axis=1) - 1
        near = jnp.sum(hits, axis=-1) > 0
        slots = jnp.where(near, near_ids * capacity + jnp.sum(slot_rank * hits, axis=-1), -1).reshape(n_micro, 2 * tokens, 2)
        near = near.reshape(n_micro, 2 * tokens, 2)
        slot_ix = jnp.arange(near_n * capacity)
        halves = [list(range(h * near_n, (h + 1) * near_n)) for h in range(2)]

        t_rank = lax.axis_index('tp')
        other_core = [(t, t ^ 1) for t in range(tp_size)]
        other_chip = [(t, t ^ 2) for t in range(tp_size)]

        def rows_of(o, k):
            return lax.dynamic_slice_in_dim(o, jnp.bitwise_xor(t_rank, k) * tokens, tokens, axis=0)

        overs, owns, sent = [], [], []
        for b in range(n_micro):
            x_own = act_in[b] if b == 0 else after(act_in[b], first_kv)
            x_half = lax.all_gather(x_own, 'tp', axis=0, tiled=True)
            x_half = after(x_half, slots, near, peer_gates) if b == 0 else after(x_half, sent[b - 1])
            kv = dot(x_half, wkv, BF16)
            if b == 0:
                first_kv = kv
            q = dot(after(x_half, kv), wq, BF16)
            kv_all = lax.all_gather(kv, 'cp', axis=0)
            o = attend(rank, q, kv_all, cp_size, heads)
            give = dot(jnp.concatenate([rows_of(o, 3), rows_of(o, 1)], axis=0), wo)
            got = lax.ppermute(give, 'tp', other_core)
            keep = dot(jnp.concatenate([rows_of(after(o, give), 2), rows_of(after(o, give), 0)], axis=0), wo)
            sent.append(keep[:tokens] + got[:tokens])
            overs.append(lax.ppermute(sent[b], 'tp', other_chip))
            owns.append(keep[tokens:] + got[tokens:])

        mids, peers = [], []
        for b in range(n_micro):
            over = after(overs[b], sent[-1]) if b == 0 else after(overs[b], mids[b - 1])
            mids.append((act_in[b].astype(F32) + (owns[b] + over)).astype(BF16))
            peers.append(lax.ppermute(mids[b], 'cp', swap))

        def pick_of(b, choice):
            return (slots[b, :, choice][:, None] == slot_ix[None, :]).astype(BF16)

        pairs, sends = [], []
        for b in range(n_micro):
            peer = after(peers[b], mids[-1] if b == 0 else sends[b - 1])
            pairs.append(jnp.concatenate([mids[b], peer], axis=0))
            pick = ((slots[b, :, 0][None, :] == slot_ix[:, None]) | (slots[b, :, 1][None, :] == slot_ix[:, None])).astype(BF16)
            sends.append(dot(pick, pairs[b], BF16))
        results = []
        for b in range(n_micro):
            expert_in = lax.all_to_all(sends[b], group, 0, 0, tiled=True, axis_index_groups=halves)
            expert_in = after(expert_in, sends[-1] if b == 0 else results[b - 1])
            gate_act = dot(expert_in, w_gate[0])
            up_act = dot(expert_in, w_up[0])
            mixed = (jax.nn.silu(gate_act) * up_act).astype(BF16)
            results.append(dot(mixed, w_down[0], BF16))
        near_rows, far_rows = [], []
        for b in range(n_micro):
            back = lax.all_to_all(results[b], group, 0, 0, tiled=True, axis_index_groups=halves)
            back = after(back, results[-1] if b == 0 else far_rows[b - 1])
            z0 = dot(pick_of(b, 0), back)
            z1 = dot(pick_of(b, 1), back)
            near_rows.append((z0[:tokens], z1[:tokens]))
            p0, p1 = z0[tokens:], z1[tokens:]
            both = near[b, tokens:, 0:1] & near[b, tokens:, 1:2]
            gates = peer_gates[b]
            full = pairs[b][tokens:].astype(F32) + (gates[:, 0:1] * p0 + gates[:, 1:2] * p1)
            far_rows.append(jnp.where(both, full, p0 + p1).astype(BF16))
        outs = []
        for b in range(n_micro):
            far = lax.ppermute(far_rows[b], 'cp', swap)
            far = after(far, far_rows[-1] if b == 0 else outs[b - 1])
            n0, n1 = near[b, :tokens, 0:1], near[b, :tokens, 1:2]
            gates = route_gates[b]
            far_row = far.astype(F32)
            c0 = jnp.where(n0, near_rows[b][0], far_row)
            c1 = jnp.where(n1, near_rows[b][1], far_row)
            mine = (mids[b].astype(F32) + (gates[:, 0:1] * c0 + gates[:, 1:2] * c1)).astype(BF16)
            outs.append(jnp.where(n0 | n1, mine, far))
        return jnp.stack(outs)

    return jax.shard_map(device_step, mesh=mesh, in_specs=(row_spec, row_spec, row_spec, head_spec, head_spec, head_spec, out_spec, expert_spec, expert_spec, expert_spec), out_specs=row_spec, check_vma=False)
```

```python
import jax
import jax.numpy as jnp
from jax import lax
from jax.experimental import pallas as pl
from jax.experimental.pallas import tpu as pltpu
from jax.sharding import PartitionSpec as P


F32, BF16 = jnp.float32, jnp.bfloat16


def attend_kernel(cp_size, heads, rank_ref, q_ref, kv_ref, o_ref, vt_ref, acc_ref):
    piece, dim = q_ref.shape[0] // 2, q_ref.shape[1] // heads
    pieces = 2 * cp_size
    scale = dim ** -0.5
    for j in range(pieces):
        owner, half = (j, 0) if j < cp_size else (pieces - 1 - j, 1)
        vt_ref[j] = kv_ref[owner, half * piece:(half + 1) * piece, dim:].T
    rank = rank_ref[0]

    def keys_of(j):
        owner = jnp.where(j < cp_size, j, pieces - 1 - j)
        start = jnp.where(j < cp_size, 0, piece)
        return kv_ref[owner, pl.ds(pl.multiple_of(start, piece), piece), 0:dim]

    key_ix = lax.broadcasted_iota(jnp.int32, (piece, piece), 0)
    query_ix = lax.broadcasted_iota(jnp.int32, (piece, piece), 1)
    keep_one = key_ix <= query_ix

    def run(half, first, count):
        last = jnp.where(half == 0, rank, pieces - 1 - rank)
        rows = pl.ds(pl.multiple_of(half * piece, piece), piece)
        lanes = [pl.ds(pl.multiple_of((first + n) * dim, dim), dim) for n in range(count)]
        cols = count * piece
        qt = jnp.concatenate([q_ref[rows, ln].T for ln in lanes], axis=1)
        keep = jnp.concatenate([keep_one] * count, axis=1)
        s = jnp.dot(keys_of(last), qt, preferred_element_type=F32) * scale
        s = jnp.where(keep, s, -jnp.inf)
        peak = jnp.max(s, axis=0, keepdims=True)
        e = jnp.exp(s - peak)
        total = jnp.sum(e, axis=0, keepdims=True)
        acc_ref[:, 0:cols] = jnp.dot(vt_ref[last], e.astype(BF16), preferred_element_type=F32)

        def step(j, carry):
            peak, total = carry
            s = jnp.dot(keys_of(j), qt, preferred_element_type=F32) * scale
            new_peak = jnp.maximum(peak, jnp.max(s, axis=0, keepdims=True))
            e = jnp.exp(s - new_peak)
            shrink = jnp.exp(peak - new_peak)
            total = total * shrink + jnp.sum(e, axis=0, keepdims=True)
            acc_ref[:, 0:cols] = acc_ref[:, 0:cols] * shrink + jnp.dot(vt_ref[j], e.astype(BF16), preferred_element_type=F32)
            return new_peak, total

        peak, total = lax.fori_loop(0, last, step, (peak, total))
        out = (acc_ref[:, 0:cols] / total).T.astype(BF16)
        for n, ln in enumerate(lanes):
            o_ref[rows, ln] = out[n * piece:(n + 1) * piece]

    twos = heads // 2

    def run_two(i, _):
        run(i // twos, i % twos * 2, 2)
        return 0

    lax.fori_loop(0, 2 * twos, run_two, 0)
    if heads % 2:
        def run_one(half, _):
            run(half, heads - 1, 1)
            return 0

        lax.fori_loop(0, 2, run_one, 0)


def attend(rank, q, kv, cp_size, heads):
    rows, width = q.shape
    dim = width // heads
    vmem = pl.BlockSpec(memory_space=pltpu.VMEM)
    pairs = heads * (rows // 2) ** 2 * (2 * cp_size + 1)
    return pl.pallas_call(
        lambda *refs: attend_kernel(cp_size, heads, *refs),
        out_shape=jax.ShapeDtypeStruct(q.shape, BF16),
        in_specs=[pl.BlockSpec(memory_space=pltpu.SMEM), vmem, vmem],
        out_specs=vmem,
        scratch_shapes=[pltpu.VMEM((2 * cp_size, dim, rows // 2), BF16), pltpu.VMEM((dim, rows), F32)],
        cost_estimate=pl.CostEstimate(flops=6 * dim * pairs, bytes_accessed=4 * q.size + 2 * kv.size, transcendentals=pairs),
        compiler_params=pltpu.CompilerParams(vmem_limit_bytes=24 * 2 ** 20),
    )(rank, q, kv)


def expert_kernel(steps, x_ref, gate_ref, up_ref, down_ref, o_ref, mixed_ref):
    i = pl.program_id(0)
    width = gate_ref.shape[2]

    @pl.when(i < steps)
    def _():
        gate = jnp.dot(x_ref[...], gate_ref[0], preferred_element_type=F32)
        up = jnp.dot(x_ref[...], up_ref[0], preferred_element_type=F32)
        mixed_ref[:, pl.ds(pl.multiple_of(i * width, width), width)] = (jax.nn.silu(gate) * up).astype(BF16)

    @pl.when(i >= steps)
    def _():
        o_ref[...] = jnp.dot(mixed_ref[...], down_ref[0], preferred_element_type=F32).astype(BF16)


def run_expert(rows, w_gate, w_up, w_down, width=512):
    count, hidden = rows.shape
    inner = w_gate.shape[2]
    first, second = inner // width, hidden // width
    return pl.pallas_call(
        lambda *refs: expert_kernel(first, *refs),
        grid=(first + second,),
        out_shape=jax.ShapeDtypeStruct(rows.shape, BF16),
        in_specs=[
            pl.BlockSpec((count, hidden), lambda i: (0, 0)),
            pl.BlockSpec((1, hidden, width), lambda i: (0, 0, jnp.minimum(i, first - 1))),
            pl.BlockSpec((1, hidden, width), lambda i: (0, 0, jnp.minimum(i, first - 1))),
            pl.BlockSpec((1, inner, width), lambda i: (0, 0, jnp.maximum(i - first, 0))),
        ],
        out_specs=pl.BlockSpec((count, width), lambda i: (0, jnp.maximum(i - first, 0))),
        scratch_shapes=[pltpu.VMEM((count, inner), BF16)],
        cost_estimate=pl.CostEstimate(flops=6 * count * hidden * inner, bytes_accessed=6 * hidden * inner + 4 * count * hidden, transcendentals=count * inner),
        compiler_params=pltpu.CompilerParams(vmem_limit_bytes=44 * 2 ** 20, dimension_semantics=('arbitrary',)),
    )(rows, w_gate, w_up, w_down)


def dot(a, b, out=F32):
    return jnp.dot(a, b, preferred_element_type=F32).astype(out)


def after(value, *first):
    return lax.optimization_barrier((value,) + first)[0]


def solution(mesh):
    cp_size = mesh.shape['cp']
    tp_size = mesh.shape['tp']
    experts = cp_size * tp_size
    row_spec = P(None, ('data', 'cp', 'tp'), None)
    head_spec = P(None, 'tp', None)
    out_spec = P('tp', None, None)
    expert_spec = P(('cp', 'tp'), None, None)
    group = ('cp', 'tp')

    def device_step(act_in, route_ids, route_gates, w_query, w_key, w_value, w_out, w_gate, w_up, w_down):
        n_micro, tokens, hidden = act_in.shape
        heads, dim = w_query.shape[1], w_query.shape[2]
        rank = lax.axis_index('cp')[None].astype(jnp.int32)
        wq = w_query.reshape(hidden, heads * dim)
        wkv = jnp.concatenate([w_key.reshape(hidden, dim), w_value.reshape(hidden, dim)], axis=1)
        wo = w_out.reshape(heads * dim, hidden)

        choices = 2 * tokens
        near_n = experts // 2
        capacity = 2 * choices // experts
        half_id = lax.axis_index('cp') // (cp_size // 2)
        swap = [(i, (i + cp_size // 2) % cp_size) for i in range(cp_size)]
        peer_gates = lax.ppermute(route_gates, 'cp', swap)
        both_ids = jnp.stack([route_ids, lax.ppermute(route_ids, 'cp', swap)])
        near_ids = both_ids.reshape(2 * n_micro, choices) - half_id * near_n
        hits = (near_ids[..., None] == jnp.arange(near_n)).astype(jnp.int32)
        slot_rank = jnp.cumsum(hits, axis=1) - 1
        near = jnp.sum(hits, axis=-1) > 0
        slots = jnp.where(near, near_ids * capacity + jnp.sum(slot_rank * hits, axis=-1), -1).reshape(2, n_micro, tokens, 2)
        near = near.reshape(2, n_micro, tokens, 2)
        slot_ix = jnp.arange(near_n * capacity)
        halves = [list(range(h * near_n, (h + 1) * near_n)) for h in range(2)]

        t_rank = lax.axis_index('tp')
        other_core = [(t, t ^ 1) for t in range(tp_size)]
        other_chip = [(t, t ^ 2) for t in range(tp_size)]

        def rows_of(o, k):
            return lax.dynamic_slice_in_dim(o, jnp.bitwise_xor(t_rank, k) * tokens, tokens, axis=0)

        overs, owns, sent = [], [], []
        for b in range(n_micro):
            x_own = act_in[b] if b == 0 else after(act_in, first_kv)[b]
            x_half = lax.all_gather(x_own, 'tp', axis=0, tiled=True)
            x_half = after(x_half, slots, near, peer_gates) if b == 0 else after(x_half, sent[b - 1])
            kv = dot(x_half, wkv, BF16)
            if b == 0:
                first_kv = kv
            q = dot(after(x_half, kv), wq, BF16)
            kv_all = lax.all_gather(kv, 'cp', axis=0)
            o = attend(rank, q, kv_all, cp_size, heads)
            give = dot(jnp.concatenate([rows_of(o, 3), rows_of(o, 1)], axis=0), wo)
            got = lax.ppermute(give, 'tp', other_core)
            keep = dot(jnp.concatenate([rows_of(after(o, give), 2), rows_of(after(o, give), 0)], axis=0), wo)
            sent.append(keep[:tokens] + got[:tokens])
            overs.append(lax.ppermute(sent[b], 'tp', other_chip))
            owns.append(keep[tokens:] + got[tokens:])

        def slot_rows(who, b, rows):
            first, second = slots[who, b, :, 0], slots[who, b, :, 1]
            return dot(((first[None, :] == slot_ix[:, None]) | (second[None, :] == slot_ix[:, None])).astype(BF16), rows, BF16)

        def exchange(rows):
            return lax.all_to_all(rows, group, 0, 0, tiled=True, axis_index_groups=halves)

        def expert(rows):
            return run_expert(rows, w_gate, w_up, w_down)

        def picked(who, b, back):
            return [dot((slots[who, b, :, k][:, None] == slot_ix[None, :]).astype(BF16), back) for k in range(2)]

        def peer_rows(b, back):
            z0, z1 = picked(1, b, back)
            both = near[1, b, :, 0:1] & near[1, b, :, 1:2]
            gates = peer_gates[b]
            full = peers[b].astype(F32) + (gates[:, 0:1] * z0 + gates[:, 1:2] * z1)
            return jnp.where(both, full, z0 + z1).astype(BF16)

        def final(b, own_back, far):
            z0, z1 = picked(0, b, own_back)
            n0, n1 = near[0, b, :, 0:1], near[0, b, :, 1:2]
            gates = route_gates[b]
            far_row = far.astype(F32)
            c0, c1 = jnp.where(n0, z0, far_row), jnp.where(n1, z1, far_row)
            mine = (mids[b].astype(F32) + (gates[:, 0:1] * c0 + gates[:, 1:2] * c1)).astype(BF16)
            return jnp.where(n0 | n1, mine, far)

        def add_back(b, over):
            return (act_in[b].astype(F32) + (owns[b] + over)).astype(BF16)

        mids, peers = [None, None], [None, None]
        mids[0] = add_back(0, after(overs[0], sent[1]))
        peers[0] = lax.ppermute(mids[0], 'cp', swap)
        own_in0 = slot_rows(0, 0, mids[0])
        lo0 = exchange(own_in0)
        peers[0] = after(peers[0], own_in0)
        peer_in0 = slot_rows(1, 0, peers[0])
        lp0 = exchange(after(peer_in0, lo0))
        mids[1] = add_back(1, after(overs[1], peer_in0))
        peers[1] = lax.ppermute(mids[1], 'cp', swap)
        own_in1 = slot_rows(0, 1, mids[1])
        lo1 = exchange(after(own_in1, lp0))
        eo0 = expert(after(lo0, own_in1))
        ep0 = expert(after(lp0, eo0))
        peers[1] = after(peers[1], ep0)
        peer_in1 = slot_rows(1, 1, peers[1])
        lp1 = exchange(after(peer_in1, lo1))
        rp0 = exchange(after(ep0, lp1))
        eo1 = expert(after(lo1, peer_in1))
        ep1 = expert(after(lp1, eo1))
        rp1 = exchange(after(ep1, rp0))
        far0 = peer_rows(0, after(rp0, ep1))
        home0 = lax.ppermute(far0, 'cp', swap)
        far1 = peer_rows(1, after(rp1, far0))
        home1 = lax.ppermute(far1, 'cp', swap)
        ro0 = exchange(after(eo0, rp1))
        ro1 = exchange(after(eo1, ro0))
        out0 = final(0, after(ro0, far1), home0)
        out1 = final(1, after(ro1, out0), home1)
        return jnp.stack([out0, out1])

    return jax.shard_map(device_step, mesh=mesh, in_specs=(row_spec, row_spec, row_spec, head_spec, head_spec, head_spec, out_spec, expert_spec, expert_spec, expert_spec), out_specs=row_spec, check_vma=False)
```
